32 devices in a mesh: dp: 8 (over z, x), expert: 4 (over y, core).
Axes of the slice: x: 2, y: 2, z: 4, core: 2. Of those that a mesh axis runs over, the one named last changes fastest.
Arguments:
- out_grad: bfloat16 [8192, 1024], P(('dp', 'expert')), may hold values from -6 to 6
- expert_of: int32 [8192, 1], P(('dp', 'expert')), may hold values from 0 to 3; in each aligned block of 256 rows (0 to 255, 256 to 511, ...) at most 128 rows name the same one
- pre_act: bfloat16 [16384, 4096], P(('dp', 'expert')), may hold values from -6 to 6
- down_weight: bfloat16 [4, 4096, 1024], P('expert', 'dp'), may hold values from -0.09375 to 0.09375
Outputs:
- pre_grad: bfloat16 [16384, 4096], P(('dp', 'expert'))
- weight_grad: float32 [4, 4096, 1024], P('expert', 'dp')
The draws below stay inside these ranges and needn't reach their ends.
Inputs may be any that keep to these rules, and one draw needn't show every extreme that they name: `expert_of`: within each aligned block of 256 rows (the rows of one device) no expert is named by more than 128 rows, and in some blocks one expert is named by exactly 128 rows.
All inputs are finite; a program needn't handle non-finite values.
Results may differ from the reference program's by a relative error of at most 0.0026.
Values may be sent and summed in bfloat16 or wider, within the bound.
A program may use at most 128 MiB of HBM per device.

```python
import math
import jax
import jax.numpy as jnp
import numpy as np
from jax import lax

D = 1024
FF = 4096
TOK_DEV = 256
CAP = 128
EXPERTS = 4
TOKENS = 8192
ROWS = 16384
N_DP = 8
N_EXPERT = 4


def raised(array, stream_key, source, target, parts, factor):
    def block_of(dim):
        return (jnp.arange(array.shape[dim]) // (array.shape[dim] // parts)).reshape((-1,) + (1,) * (array.ndim - 1 - dim))

    one_side = jax.random.permutation(stream_key, parts)[block_of(target)]
    far = (block_of(target) + parts // 2) % parts
    return jnp.where((block_of(source) == one_side) | (block_of(source) == far), factor * array, array)


def block_levels(rng, shape, shards, smallest, largest):
    def one(dim, blocks):
        draws = jax.random.uniform(jax.random.fold_in(jax.random.fold_in(rng, 6), dim), (blocks,), jnp.float32, smallest / len(shards), largest / len(shards))
        return jnp.repeat(jnp.exp(draws), shape[dim] // blocks).reshape((-1,) + (1,) * (len(shape) - dim - 1))

    loudness = one(*shards[0])
    for cut in shards[1:]:
        loudness = loudness * one(*cut)
    return loudness


def routed_block(own_key, own, number, rows, count, top, most, skew):
    sequence = jax.random.permutation(own_key, count)
    heavy_load, usual = shares(count, rows * top, most, skew, True), shares(count, rows * top, most, skew, False)
    places = jnp.arange(count)

    def named(tallies, turn):
        used = int((tallies > 0).sum())
        fixed = max(1, used // 4)
        shifted = fixed + (places - fixed + turn * (used - fixed)) % max(1, count - fixed)
        return jnp.zeros((count,), jnp.int32).at[sequence[jnp.where(places < fixed, places, shifted)]].set(jnp.asarray(tallies, jnp.int32))

    tallies = jnp.where(number % 4 == 0, named(heavy_load, number // 4), named(usual, number - number // 4 - 1))
    mixed = jax.random.permutation(jax.random.fold_in(own, 3), count)
    source_of, taker = mixed[0:count // 2 * 2:2], mixed[1:count // 2 * 2:2]
    slack = jnp.minimum(tallies[source_of] - 1, most - tallies[taker]) // 2
    slack = jnp.where((source_of == sequence[0]) | (taker == sequence[0]) | (tallies[taker] == 0), 0, jnp.maximum(slack, 0))
    shifted = jax.random.randint(jax.random.fold_in(own, 4), (count // 2,), 0, 1 << 20) % (slack + 1)
    tallies = tallies.at[source_of].add(-shifted).at[taker].add(shifted)
    labels = jnp.searchsorted(jnp.cumsum(tallies), jnp.arange(rows * top), side="right").astype(jnp.int32)
    grid = labels.reshape(top, rows).T
    grid = grid[jax.random.permutation(jax.random.fold_in(own, 1), rows)]
    turn = jax.random.randint(jax.random.fold_in(own, 2), (rows, 1), 0, top)
    return jnp.take_along_axis(grid, (jnp.arange(top)[None, :] + turn) % top, axis=1)


def shares(count, total, reach, lean, full):
    portions = [(1 << 20) // math.isqrt(rank ** lean) + 1 for rank in range(1, count + 1)]
    largest = reach if full else min(reach, max(-(-total // count), total * portions[0] // sum(portions)))
    least = 1 if total - largest >= count - 1 else 0
    counts, rest = [largest] + [least] * (count - 1), total - largest - least * (count - 1)
    while rest > 0:
        movable = [i for i in range(1, count) if counts[i] < largest] or [i for i in range(1, count) if counts[i] < reach]
        mass, budget = sum([portions[i] for i in movable]), rest
        for i in movable:
            addition = min(reach - counts[i], max(1, budget * portions[i] // mass), rest)
            counts[i] = counts[i] + addition
            rest = rest - addition
    return np.array(counts)


def gaussian(stream_key, shape, deviation, reach, cuts=(), kind=jnp.bfloat16):
    array = deviation * jax.random.normal(stream_key, shape, jnp.float32)
    if cuts:
        array = array * block_levels(stream_key, shape, cuts, -0.22, 0.18)
    return jnp.clip(array, -reach, reach).astype(kind)


def noise_with(stream_key, dims, deviation, limit, pieces, heavy, kind=jnp.bfloat16):
    values = deviation * jax.random.normal(stream_key, dims, jnp.float32)
    if pieces:
        values = values * block_levels(stream_key, dims, pieces, -0.22, 0.18)
    return jnp.clip(raised(values, jax.random.fold_in(stream_key, 3), *heavy), -limit, limit).astype(kind)


def setup_inputs(seed: int = 0) -> dict:
    keys = jax.random.split(jax.random.key(seed), 5)
    out_grad = gaussian(keys[0], (TOKENS, D), 1.0, 6.0, ((0, 32),))
    expert_of_keys = jax.random.split(jax.random.fold_in(keys[1], 1), TOKENS // TOK_DEV)
    expert_of_turns = jax.random.permutation(jax.random.fold_in(keys[1], 3), TOKENS // TOK_DEV)
    expert_of = jax.vmap(lambda own, number: routed_block(jax.random.fold_in(keys[1], 2), own, number, TOK_DEV, EXPERTS, 1, CAP, 0))(expert_of_keys, expert_of_turns).reshape((TOKENS, 1))
    pre_act = noise_with(keys[2], (ROWS, FF), 1.0, 6.0, ((0, 32),), (0, 1, 32, 2.75))
    down_weight = gaussian(keys[3], (EXPERTS, FF, D), FF ** -0.5, 0.09375, ((0, 4), (1, 8)))
    return dict(out_grad=out_grad, expert_of=expert_of, pre_act=pre_act, down_weight=down_weight)


tanh_scale = 0.7978845608028654
cubic_weight = 0.044715

def activate(values):
    argument = tanh_scale * (values + cubic_weight * values * values * values)
    return 0.5 * values * (1.0 + jnp.tanh(argument))

def derivative(values):
    tangent = jnp.tanh(tanh_scale * (values + cubic_weight * values * values * values))
    return 0.5 * (1.0 + tangent) + 0.5 * values * (1.0 - tangent * tangent) * tanh_scale * (1.0 + 3.0 * cubic_weight * values * values)

def reference(out_grad, expert_of, pre_act, down_weight):
    blocks = N_DP * N_EXPERT
    routed = expert_of[:, 0].reshape(blocks, TOK_DEV)
    onehot = (routed[:, :, None] == jnp.arange(EXPERTS, dtype=jnp.int32)[None, None, :]).astype(jnp.int32)
    position = lax.optimization_barrier(jnp.sum((jnp.cumsum(onehot, axis=1) - onehot) * onehot, axis=2))
    block_id = jnp.arange(blocks, dtype=jnp.int32)[:, None]
    replica = block_id // N_EXPERT
    source = block_id % N_EXPERT
    target = ((replica * EXPERTS + routed) * N_EXPERT + source) * CAP + position
    dispatched = jnp.zeros((ROWS, D), jnp.bfloat16).at[target.reshape(-1).astype(jnp.int32)].set(out_grad)
    grads_in = dispatched.reshape(N_DP, EXPERTS, N_EXPERT * CAP, D)
    pre_in = pre_act.reshape(N_DP, EXPERTS, N_EXPERT * CAP, FF)
    weights32 = down_weight.astype(jnp.float32)

    def accumulate(running, inputs):
        arrived, pre_rows = inputs
        pre32 = pre_rows.astype(jnp.float32)
        arrived32 = arrived.astype(jnp.float32)
        hidden_grad = jnp.einsum('erd,efd->erf', arrived32, weights32)
        pre_grad = (hidden_grad * derivative(pre32)).astype(jnp.bfloat16)
        hidden = activate(pre32).astype(jnp.bfloat16)
        partial_value = jnp.einsum('erf,erd->efd', hidden.astype(jnp.float32), arrived32)
        return (running + partial_value, pre_grad)
    running, pre_grads = lax.scan(accumulate, jnp.zeros((EXPERTS, FF, D), jnp.float32), (grads_in, pre_in))
    factor = jnp.float32(1.0 / math.sqrt(N_DP * TOK_DEV))
    return (pre_grads.reshape(ROWS, FF), running * factor)
```

```python
import functools
import math

import jax
import jax.numpy as jnp
from jax import lax
from jax.experimental import pallas as pl
from jax.experimental.pallas import tpu as pltpu
from jax.sharding import PartitionSpec as P

tanh_scale = 0.7978845608028654
cubic_weight = 0.044715
MESH = pl.DeviceIdType.MESH
PAIR = 2
LINE = 4
CUTS = 2


def activate(values):
    argument = tanh_scale * (values + cubic_weight * values * values * values)
    return 0.5 * values * (1.0 + jnp.tanh(argument))


def derivative(values):
    tangent = jnp.tanh(tanh_scale * (values + cubic_weight * values * values * values))
    return 0.5 * (1.0 + tangent) + 0.5 * values * (1.0 - tangent * tangent) * tanh_scale * (
        1.0 + 3.0 * cubic_weight * values * values
    )


def kernel(
    experts,
    capacity,
    factor,
    tokens_ref,
    route_ref,
    pre_hbm,
    weight_hbm,
    grad_hbm,
    dw_ref,
    their_tokens,
    their_route,
    outgoing,
    arrived,
    pre_own,
    pre_theirs,
    weights,
    hidden,
    slope,
    partial,
    sums_out,
    sums_in,
    grad_own,
    grad_theirs,
    token_sems,
    send_sems,
    arrive_sems,
    local_sems,
    pre_sems,
    weight_send,
    weight_recv,
    sum_send,
    sum_recv,
    grad_sems,
):
    d = lax.axis_index("dp")
    me = lax.axis_index("expert")
    z = lax.div(d, PAIR)
    x = lax.rem(d, PAIR)
    partner = z * PAIR + 1 - x
    rows, width = pre_hbm.shape[0], tokens_ref.shape[1]
    block = weight_hbm.shape[0]
    count = tokens_ref.shape[0]
    low = z < LINE // 2

    def order(i):
        if i == LINE - 1:
            return z
        down = LINE - 1 - i
        return jnp.where(
            low, jnp.where(down > z, down, down - 1), jnp.where(i < z, i, i + 1)
        )

    def columns(j, side):
        return pl.ds(pl.multiple_of((j * PAIR + side) * block, block), block)

    barrier = pltpu.get_barrier_semaphore()
    pl.semaphore_signal(barrier, inc=1, device_id={"dp": partner}, device_id_type=MESH)
    for k in range(1, experts):
        pl.semaphore_signal(
            barrier, inc=1, device_id={"expert": lax.rem(me + k, experts)}, device_id_type=MESH
        )

    @pl.when(z > 0)
    def _():
        pl.semaphore_signal(barrier, inc=1, device_id={"dp": d - PAIR}, device_id_type=MESH)

    @pl.when(z < LINE - 1)
    def _():
        pl.semaphore_signal(barrier, inc=1, device_id={"dp": d + PAIR}, device_id_type=MESH)

    inner = jnp.where((z > 0) & (z < LINE - 1), 2, 1)
    pl.semaphore_wait(barrier, experts + inner)

    def remote(src, dst, send, recv, device):
        return pltpu.make_async_remote_copy(
            src_ref=src, dst_ref=dst, send_sem=send, recv_sem=recv,
            device_id=device, device_id_type=MESH,
        )

    route_copy = remote(
        route_ref, their_route, token_sems.at[0], token_sems.at[1], {"dp": partner}
    )
    token_copy = remote(
        tokens_ref, their_tokens, token_sems.at[2], token_sems.at[3], {"dp": partner}
    )
    route_copy.start()
    token_copy.start()

    def weight_copy(direction, hop):
        step = 1 - 2 * direction
        shard = z - step * hop
        shard = jnp.clip(shard, 0, LINE - 1)
        src = weight_hbm if hop == 0 else weights.at[shard]
        return remote(
            src, weights.at[shard], weight_send.at[direction, hop],
            weight_recv.at[direction, hop], {"dp": d + step * PAIR},
        )

    def sends(direction, hop):
        if direction == 0:
            return (z >= hop) & (z < LINE - 1)
        return (z <= LINE - 1 - hop) & (z > 0)

    def receives(direction, hop):
        return (z > hop) if direction == 0 else (z < LINE - 1 - hop)

    def weight_start(hop):
        for direction in range(2):
            @pl.when(sends(direction, hop))
            def _():
                weight_copy(direction, hop).start()

    def weight_arrive(hop):
        for direction in range(2):
            @pl.when(receives(direction, hop))
            def _():
                step = 1 - 2 * direction
                shard = jnp.clip(z - step * (hop + 1), 0, LINE - 1)
                remote(
                    weight_hbm, weights.at[shard], weight_send.at[direction, hop],
                    weight_recv.at[direction, hop], {"dp": partner},
                ).wait_recv()

    weight_start(0)

    def pre_copy(i):
        return remote(
            pre_hbm.at[:, columns(order(i), 1 - x)], pre_theirs.at[i],
            pre_sems.at[0, i], pre_sems.at[1, i], {"dp": partner},
        )

    for i in range(LINE):
        pre_copy(i).start()

    def own_copy(i):
        return pltpu.make_async_copy(
            pre_hbm.at[:, columns(order(i), x)], pre_own.at[i], local_sems.at[i]
        )

    for i in range(LINE):
        own_copy(i).start()
    weight_own = pltpu.make_async_copy(weight_hbm, weights.at[z], local_sems.at[LINE])
    weight_own.start()

    def slots(source):
        return pl.ds(pl.multiple_of(source * capacity, capacity), capacity)

    def arrival(rep, k):
        source = lax.rem(me + experts - k, experts)
        return remote(
            outgoing.at[rep, k - 1],
            arrived.at[rep, slots(source)],
            send_sems.at[rep, k - 1],
            arrive_sems.at[rep, k - 1],
            {"expert": lax.rem(me + k, experts)},
        )

    earlier = (
        lax.broadcasted_iota(jnp.int32, (count, count), 0)
        < lax.broadcasted_iota(jnp.int32, (count, count), 1)
    ).astype(jnp.float32).astype(jnp.bfloat16)

    def dispatch(rep, routes, tokens):
        names = routes[...]
        named = lax.broadcasted_iota(jnp.int32, (8, count), 0) == names
        onehot = named.astype(jnp.float32)
        before = jnp.dot(
            onehot.astype(jnp.bfloat16), earlier, preferred_element_type=jnp.float32
        )
        position = jnp.sum(onehot * before, axis=0, keepdims=True).astype(jnp.int32)
        slot = lax.broadcasted_iota(jnp.int32, (capacity, count), 0)
        for k in list(range(1, experts)) + [0]:
            target = lax.rem(me + k, experts)
            place = jnp.where(names == target, position, -1)
            choose = (slot == place).astype(jnp.float32).astype(jnp.bfloat16)
            rows_out = jnp.dot(
                choose, tokens[...], preferred_element_type=jnp.float32
            ).astype(jnp.bfloat16)
            if k == 0:
                arrived[rep, slots(me), :] = rows_out
            else:
                outgoing[rep, k - 1] = rows_out
                remote(
                    outgoing.at[rep, k - 1],
                    arrived.at[rep, slots(me)],
                    send_sems.at[rep, k - 1],
                    arrive_sems.at[rep, k - 1],
                    {"expert": target},
                ).start()

    dispatch(0, route_ref, tokens_ref)

    strip = 64

    def activate_rows(rep, i, source):
        @pl.loop(0, rows // (2 * strip))
        def _(t):
            for half in range(2):
                at = pl.ds(pl.multiple_of(t * 2 * strip + half * strip, strip), strip)
                v = source[i, at, :].astype(jnp.float32)
                square = v * v
                tangent = jnp.tanh(tanh_scale * v * (1.0 + cubic_weight * square))
                gate = 0.5 * (1.0 + tangent)
                slope[rep, i, at, :] = gate + 0.5 * v * (1.0 - tangent * tangent) * tanh_scale * (
                    1.0 + 3.0 * cubic_weight * square
                )
                hidden[rep, i, at, :] = (v * gate).astype(jnp.bfloat16)

    route_copy.wait_recv()
    token_copy.wait_recv()
    dispatch(1, their_route, their_tokens)
    for i in range(LINE):
        own_copy(i).wait()
        activate_rows(0, i, pre_own)

    weight_arrive(0)
    weight_start(1)
    for rep in range(2):
        for k in range(1, experts):
            arrival(rep, k).wait_recv()

    tile = 256

    def multiply(i):
        pre_copy(i).wait_recv()
        activate_rows(1, i, pre_theirs)

        @pl.loop(0, block // tile)
        def _(t):
            at = pl.ds(pl.multiple_of(t * tile, tile), tile)
            total = lax.dot_general(
                hidden[0, i, :, at], arrived[0], (((0,), (0,)), ((), ())),
                preferred_element_type=jnp.float32,
            )
            partial[i, at, :] = total + lax.dot_general(
                hidden[1, i, :, at], arrived[1], (((0,), (0,)), ((), ())),
                preferred_element_type=jnp.float32,
            )

    piece = block // CUTS

    def sum_copy(direction, stage, cut):
        part = pl.ds(cut * piece, piece)
        return remote(
            sums_out.at[direction, stage, part], sums_in.at[direction, stage, part],
            sum_send.at[direction, stage, cut], sum_recv.at[direction, stage, cut],
            {"dp": d + (1 - 2 * direction) * PAIR},
        )

    def pass_on(i, ends):
        j = order(i)
        for direction in range(2):
            distance = (j - z) if direction == 0 else (z - j)
            first = (z == 0) if direction == 0 else (z == LINE - 1)
            stage = jnp.clip(LINE - 1 - distance, 0, LINE - 2)
            if ends:
                @pl.when((distance > 0) & first)
                def _():
                    for cut in range(CUTS):
                        part = pl.ds(cut * piece, piece)
                        sums_out[direction, stage, part, :] = partial[i, part, :].astype(
                            jnp.bfloat16
                        )
                        sum_copy(direction, stage, cut).start()
            else:
                @pl.when((distance > 0) & jnp.logical_not(first))
                def _():
                    last = jnp.clip(stage - 1, 0, LINE - 2)
                    for cut in range(CUTS):
                        part = pl.ds(cut * piece, piece)
                        sum_copy(direction, last, cut).wait_recv()
                        sums_out[direction, stage, part, :] = (
                            partial[i, part, :]
                            + sums_in[direction, last, part, :].astype(jnp.float32)
                        ).astype(jnp.bfloat16)
                        sum_copy(direction, stage, cut).start()

    def grad_copy(i):
        return remote(
            grad_theirs.at[i], grad_hbm.at[:, columns(order(i), x)],
            grad_sems.at[0, i], grad_sems.at[1, i], {"dp": partner},
        )

    def grad_arrive(i):
        return remote(
            grad_theirs.at[i], grad_hbm.at[:, columns(order(i), 1 - x)],
            grad_sems.at[0, i], grad_sems.at[1, i], {"dp": partner},
        )

    def grad_write(i):
        return pltpu.make_async_copy(
            grad_own.at[i], grad_hbm.at[:, columns(order(i), x)], grad_sems.at[2, i]
        )

    def differentiate(i):
        j = order(i)
        for rep, result in ((1, grad_theirs), (0, grad_own)):
            @pl.loop(0, rows // tile)
            def _(t):
                at = pl.ds(pl.multiple_of(t * tile, tile), tile)
                product = lax.dot_general(
                    arrived[rep, at, :], weights[j], (((1,), (1,)), ((), ())),
                    preferred_element_type=jnp.float32,
                )
                result[i, at, :] = (product * slope[rep, i, at, :]).astype(jnp.bfloat16)

            if rep == 1:
                grad_copy(i).start()
            else:
                grad_write(i).start()

    multiply(0)
    pass_on(0, True)
    multiply(1)
    pass_on(1, True)
    weight_arrive(1)
    weight_start(2)
    weight_own.wait()
    pass_on(0, False)
    multiply(2)
    pass_on(2, True)
    differentiate(2)
    differentiate(1)
    multiply(3)
    differentiate(3)
    weight_arrive(2)
    differentiate(0)
    pass_on(1, False)
    pass_on(2, False)

    for cut in range(CUTS):
        part = pl.ds(cut * piece, piece)
        dw_ref[part, :] = partial[LINE - 1, part, :]
        for direction in range(2):
            @pl.when(receives(direction, 0))
            def _():
                sum_copy(direction, LINE - 2, cut).wait_recv()
                dw_ref[part, :] += sums_in[direction, LINE - 2, part, :].astype(jnp.float32)
        dw_ref[part, :] = dw_ref[part, :] * factor

    for i in range(LINE):
        grad_arrive(i).wait_recv()
        grad_write(i).wait()
    route_copy.wait_send()
    token_copy.wait_send()
    for i in range(LINE):
        pre_copy(i).wait_send()
        grad_copy(i).wait_send()
    for rep in range(2):
        for k in range(1, experts):
            arrival(rep, k).wait_send()
    for hop in range(LINE - 1):
        for direction in range(2):
            @pl.when(sends(direction, hop))
            def _():
                weight_copy(direction, hop).wait_send()
    for stage in range(LINE - 1):
        for direction in range(2):
            toward = (z <= stage) if direction == 0 else (z >= LINE - 1 - stage)
            inside = (z < LINE - 1) if direction == 0 else (z > 0)

            @pl.when(toward & inside)
            def _():
                for cut in range(CUTS):
                    sum_copy(direction, stage, cut).wait_send()


def fused(out_grad, expert_of, pre_act, down_weight):
    experts = lax.axis_size("expert")
    replicas = lax.axis_size("dp")
    count, width = out_grad.shape
    rows, units = pre_act.shape
    block = down_weight.shape[1]
    capacity = count // 2
    factor = 1.0 / math.sqrt(replicas * count)
    half, full = jnp.bfloat16, jnp.float32
    vmem = pl.BlockSpec(memory_space=pltpu.VMEM)
    anywhere = pl.BlockSpec(memory_space=pl.ANY)
    dma = pltpu.SemaphoreType.DMA
    pre_grad, summed = pl.pallas_call(
        functools.partial(kernel, experts, capacity, factor),
        out_shape=(
            jax.ShapeDtypeStruct((rows, units), half),
            jax.ShapeDtypeStruct((block, width), full),
        ),
        in_specs=[vmem, vmem, anywhere, anywhere],
        out_specs=(anywhere, vmem),
        scratch_shapes=[
            pltpu.VMEM((count, width), half),
            pltpu.VMEM((1, count), jnp.int32),
            pltpu.VMEM((2, experts - 1, capacity, width), half),
            pltpu.VMEM((2, rows, width), half),
            pltpu.VMEM((LINE, rows, block), half),
            pltpu.VMEM((LINE, rows, block), half),
            pltpu.VMEM((LINE, block, width), half),
            pltpu.VMEM((2, LINE, rows, block), half),
            pltpu.VMEM((2, LINE, rows, block), full),
            pltpu.VMEM((LINE, block, width), full),
            pltpu.VMEM((2, LINE - 1, block, width), half),
            pltpu.VMEM((2, LINE - 1, block, width), half),
            pltpu.VMEM((LINE, rows, block), half),
            pltpu.VMEM((LINE, rows, block), half),
            dma((4,)),
            dma((2, experts - 1)),
            dma((2, experts - 1)),
            dma((LINE + 1,)),
            dma((2, LINE)),
            dma((2, LINE - 1)),
            dma((2, LINE - 1)),
            dma((2, LINE - 1, CUTS)),
            dma((2, LINE - 1, CUTS)),
            dma((3, LINE)),
        ],
        compiler_params=pltpu.CompilerParams(
            collective_id=0, has_side_effects=True, vmem_limit_bytes=60 * 1024 * 1024
        ),
    )(out_grad, expert_of.reshape(1, count), pre_act, down_weight[0])
    return pre_grad, summed.reshape(1, block, width)


def body(out_grad, expert_of, pre_act, down_weight):
    experts = lax.axis_size("expert")
    replicas = lax.axis_size("dp")
    if replicas == PAIR * LINE and experts <= 8:
        return fused(out_grad, expert_of, pre_act, down_weight)
    token_count = out_grad.shape[0]
    model_width = out_grad.shape[1]
    capacity = token_count // 2
    routed = expert_of[:, 0]
    onehot = (routed[:, None] == jnp.arange(experts, dtype=jnp.int32)[None, :]).astype(jnp.int32)
    position = jnp.sum((jnp.cumsum(onehot, axis=0) - onehot) * onehot, axis=1)
    target = routed * capacity + position
    outgoing = jnp.zeros((experts * capacity, model_width), jnp.bfloat16).at[target].set(out_grad)
    arrived = lax.all_to_all(
        outgoing.reshape(experts, capacity, model_width),
        "expert",
        split_axis=0,
        concat_axis=0,
        tiled=True,
    )
    arrived = arrived.reshape(experts * capacity, model_width)
    weight = down_weight[0]
    own_rows = weight.shape[0]
    factor = 1.0 / math.sqrt(replicas * token_count)
    hidden_grad = lax.dot_general(
        arrived,
        lax.all_gather(weight, "dp", axis=0, tiled=True),
        (((1,), (1,)), ((), ())),
        preferred_element_type=jnp.float32,
    )
    pre_block = pre_act.astype(jnp.float32)
    pre_grad = (hidden_grad * derivative(pre_block)).astype(jnp.bfloat16)
    hidden = activate(pre_block).astype(jnp.bfloat16)
    summed = lax.psum_scatter(
        lax.dot_general(
            hidden, arrived, (((0,), (0,)), ((), ())), preferred_element_type=jnp.float32
        ),
        "dp",
        scatter_dimension=0,
        tiled=True,
    )
    return (pre_grad, (summed * factor).reshape(1, own_rows, model_width))


def solution(mesh):
    placed = (
        P(("dp", "expert"), None),
        P(("dp", "expert"), None),
        P(("dp", "expert"), None),
        P("expert", "dp", None),
    )
    return jax.shard_map(
        body,
        mesh=mesh,
        in_specs=placed,
        out_specs=(P(("dp", "expert"), None), P("expert", "dp", None)),
        check_vma=False,
    )
```

```python
import functools
import math

import jax
import jax.numpy as jnp
from jax import lax
from jax.experimental import pallas as pl
from jax.experimental.pallas import tpu as pltpu
from jax.sharding import PartitionSpec as P

tanh_scale = 0.7978845608028654
cubic_weight = 0.044715
MESH = pl.DeviceIdType.MESH
PAIR = 2
LINE = 4
CUTS = 2


def activate(values):
    argument = tanh_scale * (values + cubic_weight * values * values * values)
    return 0.5 * values * (1.0 + jnp.tanh(argument))


def derivative(values):
    tangent = jnp.tanh(tanh_scale * (values + cubic_weight * values * values * values))
    return 0.5 * (1.0 + tangent) + 0.5 * values * (1.0 - tangent * tangent) * tanh_scale * (
        1.0 + 3.0 * cubic_weight * values * values
    )


def kernel(
    experts,
    capacity,
    factor,
    tokens_ref,
    route_ref,
    pre_hbm,
    weight_hbm,
    grad_hbm,
    dw_hbm,
    their_tokens,
    their_route,
    outgoing,
    arrived,
    pre_own,
    pre_theirs,
    weights,
    hidden,
    slope,
    partial,
    sums_out,
    sums_in,
    token_sems,
    send_sems,
    arrive_sems,
    local_sems,
    pre_sems,
    weight_send,
    weight_recv,
    sum_send,
    sum_recv,
    grad_sems,
):
    d = lax.axis_index("dp")
    me = lax.axis_index("expert")
    z = lax.div(d, PAIR)
    x = lax.rem(d, PAIR)
    partner = z * PAIR + 1 - x
    rows, width = pre_hbm.shape[0], tokens_ref.shape[1]
    block = weight_hbm.shape[0]
    count = tokens_ref.shape[0]
    low = z < LINE // 2

    def order(i):
        if i == LINE - 1:
            return z
        down = LINE - 1 - i
        return jnp.where(
            low, jnp.where(down > z, down, down - 1), jnp.where(i < z, i, i + 1)
        )

    piece = block // CUTS

    def columns(j, side):
        return pl.ds(pl.multiple_of((j * PAIR + side) * block, block), block)

    def within(cut):
        return pl.ds(pl.multiple_of(cut * piece, piece), piece)

    barrier = pltpu.get_barrier_semaphore()
    pl.semaphore_signal(barrier, inc=1, device_id={"dp": partner}, device_id_type=MESH)
    for k in range(1, experts):
        pl.semaphore_signal(
            barrier, inc=1, device_id={"expert": lax.rem(me + k, experts)}, device_id_type=MESH
        )

    @pl.when(z > 0)
    def _():
        pl.semaphore_signal(barrier, inc=1, device_id={"dp": d - PAIR}, device_id_type=MESH)

    @pl.when(z < LINE - 1)
    def _():
        pl.semaphore_signal(barrier, inc=1, device_id={"dp": d + PAIR}, device_id_type=MESH)

    inner = jnp.where((z > 0) & (z < LINE - 1), 2, 1)
    pl.semaphore_wait(barrier, experts + inner)

    def remote(src, dst, send, recv, device):
        return pltpu.make_async_remote_copy(
            src_ref=src, dst_ref=dst, send_sem=send, recv_sem=recv,
            device_id=device, device_id_type=MESH,
        )

    route_copy = remote(
        route_ref, their_route, token_sems.at[0], token_sems.at[1], {"dp": partner}
    )
    token_copy = remote(
        tokens_ref, their_tokens, token_sems.at[2], token_sems.at[3], {"dp": partner}
    )
    route_copy.start()
    token_copy.start()

    def weight_copy(direction, hop):
        step = 1 - 2 * direction
        shard = z - step * hop
        shard = jnp.clip(shard, 0, LINE - 1)
        src = weight_hbm if hop == 0 else weights.at[shard]
        return remote(
            src, weights.at[shard], weight_send.at[direction, hop],
            weight_recv.at[direction, hop], {"dp": d + step * PAIR},
        )

    def sends(direction, hop):
        if direction == 0:
            return (z >= hop) & (z < LINE - 1)
        return (z <= LINE - 1 - hop) & (z > 0)

    def receives(direction, hop):
        return (z > hop) if direction == 0 else (z < LINE - 1 - hop)

    def weight_start(hop):
        for direction in range(2):
            @pl.when(sends(direction, hop))
            def _():
                weight_copy(direction, hop).start()

    def weight_arrive(hop):
        for direction in range(2):
            @pl.when(receives(direction, hop))
            def _():
                step = 1 - 2 * direction
                shard = jnp.clip(z - step * (hop + 1), 0, LINE - 1)
                remote(
                    weight_hbm, weights.at[shard], weight_send.at[direction, hop],
                    weight_recv.at[direction, hop], {"dp": partner},
                ).wait_recv()

    weight_start(0)

    def pre_copy(i, cut):
        start = (order(i) * PAIR + 1 - x) * block + cut * piece
        return remote(
            pre_hbm.at[:, pl.ds(pl.multiple_of(start, piece), piece)],
            pre_theirs.at[i, :, within(cut)],
            pre_sems.at[0, i, cut], pre_sems.at[1, i, cut], {"dp": partner},
        )

    for i in range(LINE):
        for cut in range(CUTS):
            pre_copy(i, cut).start()

    def own_copy(i):
        return pltpu.make_async_copy(
            pre_hbm.at[:, columns(order(i), x)], pre_own.at[i], local_sems.at[i]
        )

    for i in range(LINE):
        own_copy(i).start()
    weight_own = pltpu.make_async_copy(weight_hbm, weights.at[z], local_sems.at[LINE])
    weight_own.start()

    def slots(source):
        return pl.ds(pl.multiple_of(source * capacity, capacity), capacity)

    def arrival(rep, k):
        source = lax.rem(me + experts - k, experts)
        return remote(
            outgoing.at[rep, k - 1],
            arrived.at[rep, slots(source)],
            send_sems.at[rep, k - 1],
            arrive_sems.at[rep, k - 1],
            {"expert": lax.rem(me + k, experts)},
        )

    earlier = (
        lax.broadcasted_iota(jnp.int32, (count, count), 0)
        < lax.broadcasted_iota(jnp.int32, (count, count), 1)
    ).astype(jnp.float32).astype(jnp.bfloat16)

    def dispatch(rep, routes, tokens):
        names = routes[...]
        named = lax.broadcasted_iota(jnp.int32, (8, count), 0) == names
        onehot = named.astype(jnp.float32)
        before = jnp.dot(
            onehot.astype(jnp.bfloat16), earlier, preferred_element_type=jnp.float32
        )
        position = jnp.sum(onehot * before, axis=0, keepdims=True).astype(jnp.int32)
        slot = lax.broadcasted_iota(jnp.int32, (capacity, count), 0)
        for k in list(range(1, experts)) + [0]:
            target = lax.rem(me + k, experts)
            place = jnp.where(names == target, position, -1)
            choose = (slot == place).astype(jnp.float32).astype(jnp.bfloat16)
            rows_out = jnp.dot(
                choose, tokens[...], preferred_element_type=jnp.float32
            ).astype(jnp.bfloat16)
            if k == 0:
                arrived[rep, slots(me), :] = rows_out
            else:
                outgoing[rep, k - 1] = rows_out
                remote(
                    outgoing.at[rep, k - 1],
                    arrived.at[rep, slots(me)],
                    send_sems.at[rep, k - 1],
                    arrive_sems.at[rep, k - 1],
                    {"expert": target},
                ).start()

    dispatch(0, route_ref, tokens_ref)

    strip = 64

    def activate_rows(rep, i, source, cut):
        at_columns = within(cut)

        @pl.loop(0, rows // (2 * strip))
        def _(t):
            for half in range(2):
                at = pl.ds(pl.multiple_of(t * 2 * strip + half * strip, strip), strip)
                v = source[i, at, at_columns].astype(jnp.float32)
                square = v * v
                tangent = jnp.tanh(tanh_scale * v * (1.0 + cubic_weight * square))
                gate = 0.5 * (1.0 + tangent)
                slope[rep, i, at, at_columns] = gate + 0.5 * v * (
                    1.0 - tangent * tangent
                ) * tanh_scale * (1.0 + 3.0 * cubic_weight * square)
                hidden[rep, i, at, at_columns] = (v * gate).astype(jnp.bfloat16)

    route_copy.wait_recv()
    token_copy.wait_recv()
    dispatch(1, their_route, their_tokens)
    for i in range(LINE):
        own_copy(i).wait()

        @pl.loop(0, CUTS)
        def _(cut):
            activate_rows(0, i, pre_own, cut)

    weight_arrive(0)
    weight_start(1)
    for rep in range(2):
        for k in range(1, experts):
            arrival(rep, k).wait_recv()

    tile = 256

    def multiply(i):
        @pl.loop(0, CUTS)
        def _(cut):
            pre_copy(i, cut).wait_recv()
            activate_rows(1, i, pre_theirs, cut)
            at = within(cut)
            total = lax.dot_general(
                hidden[0, i, :, at], arrived[0], (((0,), (0,)), ((), ())),
                preferred_element_type=jnp.float32,
            )
            partial[i, at, :] = total + lax.dot_general(
                hidden[1, i, :, at], arrived[1], (((0,), (0,)), ((), ())),
                preferred_element_type=jnp.float32,
            )
            if i < LINE - 1:
                pass_on(i, True, cut)

    def sum_copy(direction, stage, cut):
        part = within(cut)
        return remote(
            sums_out.at[direction, stage, part], sums_in.at[direction, stage, part],
            sum_send.at[direction, stage, cut], sum_recv.at[direction, stage, cut],
            {"dp": d + (1 - 2 * direction) * PAIR},
        )

    def pass_on(i, ends, cut):
        j = order(i)
        part = within(cut)
        for direction in range(2):
            distance = (j - z) if direction == 0 else (z - j)
            first = (z == 0) if direction == 0 else (z == LINE - 1)
            stage = jnp.clip(LINE - 1 - distance, 0, LINE - 2)
            if ends:
                @pl.when((distance > 0) & first)
                def _():
                    sums_out[direction, stage, part, :] = partial[i, part, :].astype(
                        jnp.bfloat16
                    )
                    sum_copy(direction, stage, cut).start()
            else:
                @pl.when((distance > 0) & jnp.logical_not(first))
                def _():
                    last = jnp.clip(stage - 1, 0, LINE - 2)
                    sum_copy(direction, last, cut).wait_recv()
                    sums_out[direction, stage, part, :] = (
                        partial[i, part, :]
                        + sums_in[direction, last, part, :].astype(jnp.float32)
                    ).astype(jnp.bfloat16)
                    sum_copy(direction, stage, cut).start()

    def forward(*blocks):
        @pl.loop(0, CUTS)
        def _(cut):
            for i in blocks:
                pass_on(i, False, cut)

    def grad_copy(i):
        return remote(
            pre_theirs.at[i], grad_hbm.at[:, columns(order(i), x)],
            grad_sems.at[0, i], grad_sems.at[1, i], {"dp": partner},
        )

    def grad_arrive(i):
        return remote(
            pre_theirs.at[i], grad_hbm.at[:, columns(order(i), 1 - x)],
            grad_sems.at[0, i], grad_sems.at[1, i], {"dp": partner},
        )

    def grad_write(i):
        return pltpu.make_async_copy(
            pre_own.at[i], grad_hbm.at[:, columns(order(i), x)], grad_sems.at[2, i]
        )

    def differentiate(i):
        j = order(i)
        for rep, result in ((1, pre_theirs), (0, pre_own)):
            @pl.loop(0, rows // tile)
            def _(t):
                at = pl.ds(pl.multiple_of(t * tile, tile), tile)
                product = lax.dot_general(
                    arrived[rep, at, :], weights[j], (((1,), (1,)), ((), ())),
                    preferred_element_type=jnp.float32,
                )
                result[i, at, :] = (product * slope[rep, i, at, :]).astype(jnp.bfloat16)

            if rep == 1:
                grad_copy(i).start()
            else:
                grad_write(i).start()

    multiply(0)
    multiply(1)
    weight_arrive(1)
    weight_start(2)
    weight_own.wait()
    forward(0)
    multiply(2)
    differentiate(2)
    differentiate(1)
    multiply(3)
    differentiate(3)
    weight_arrive(2)
    differentiate(0)
    forward(1, 2)

    def result_copy(cut):
        part = pl.ds(cut * piece, piece)
        return pltpu.make_async_copy(
            partial.at[LINE - 1, part], dw_hbm.at[part], local_sems.at[LINE + 1 + cut]
        )

    for cut in range(CUTS):
        part = pl.ds(cut * piece, piece)
        for direction in range(2):
            @pl.when(receives(direction, 0))
            def _():
                sum_copy(direction, LINE - 2, cut).wait_recv()
                partial[LINE - 1, part, :] += sums_in[direction, LINE - 2, part, :].astype(jnp.float32)
        partial[LINE - 1, part, :] = partial[LINE - 1, part, :] * factor
        result_copy(cut).start()

    for i in range(LINE):
        grad_arrive(i).wait_recv()
        grad_write(i).wait()
    for cut in range(CUTS):
        result_copy(cut).wait()
    route_copy.wait_send()
    token_copy.wait_send()
    for i in range(LINE):
        for cut in range(CUTS):
            pre_copy(i, cut).wait_send()
        grad_copy(i).wait_send()
    for rep in range(2):
        for k in range(1, experts):
            arrival(rep, k).wait_send()
    for hop in range(LINE - 1):
        for direction in range(2):
            @pl.when(sends(direction, hop))
            def _():
                weight_copy(direction, hop).wait_send()
    for stage in range(LINE - 1):
        for direction in range(2):
            toward = (z <= stage) if direction == 0 else (z >= LINE - 1 - stage)
            inside = (z < LINE - 1) if direction == 0 else (z > 0)

            @pl.when(toward & inside)
            def _():
                for cut in range(CUTS):
                    sum_copy(direction, stage, cut).wait_send()


def fused(out_grad, expert_of, pre_act, down_weight):
    experts = lax.axis_size("expert")
    replicas = lax.axis_size("dp")
    count, width = out_grad.shape
    rows, units = pre_act.shape
    block = down_weight.shape[1]
    capacity = count // 2
    factor = 1.0 / math.sqrt(replicas * count)
    half, full = jnp.bfloat16, jnp.float32
    vmem = pl.BlockSpec(memory_space=pltpu.VMEM)
    anywhere = pl.BlockSpec(memory_space=pl.ANY)
    dma = pltpu.SemaphoreType.DMA
    pre_grad, summed = pl.pallas_call(
        functools.partial(kernel, experts, capacity, factor),
        out_shape=(
            jax.ShapeDtypeStruct((rows, units), half),
            jax.ShapeDtypeStruct((block, width), full),
        ),
        in_specs=[vmem, vmem, anywhere, anywhere],
        out_specs=(anywhere, anywhere),
        scratch_shapes=[
            pltpu.VMEM((count, width), half),
            pltpu.VMEM((1, count), jnp.int32),
            pltpu.VMEM((2, experts - 1, capacity, width), half),
            pltpu.VMEM((2, rows, width), half),
            pltpu.VMEM((LINE, rows, block), half),
            pltpu.VMEM((LINE, rows, block), half),
            pltpu.VMEM((LINE, block, width), half),
            pltpu.VMEM((2, LINE, rows, block), half),
            pltpu.VMEM((2, LINE, rows, block), full),
            pltpu.VMEM((LINE, block, width), full),
            pltpu.VMEM((2, LINE - 1, block, width), half),
            pltpu.VMEM((2, LINE - 1, block, width), half),
            dma((4,)),
            dma((2, experts - 1)),
            dma((2, experts - 1)),
            dma((LINE + 1 + CUTS,)),
            dma((2, LINE, CUTS)),
            dma((2, LINE - 1)),
            dma((2, LINE - 1)),
            dma((2, LINE - 1, CUTS)),
            dma((2, LINE - 1, CUTS)),
            dma((3, LINE)),
        ],
        compiler_params=pltpu.CompilerParams(
            collective_id=0, has_side_effects=True, vmem_limit_bytes=46 * 1024 * 1024
        ),
    )(out_grad, expert_of.reshape(1, count), pre_act, down_weight[0])
    return pre_grad, summed.reshape(1, block, width)


def body(out_grad, expert_of, pre_act, down_weight):
    experts = lax.axis_size("expert")
    replicas = lax.axis_size("dp")
    if replicas == PAIR * LINE and experts <= 8:
        return fused(out_grad, expert_of, pre_act, down_weight)
    token_count = out_grad.shape[0]
    model_width = out_grad.shape[1]
    capacity = token_count // 2
    routed = expert_of[:, 0]
    onehot = (routed[:, None] == jnp.arange(experts, dtype=jnp.int32)[None, :]).astype(jnp.int32)
    position = jnp.sum((jnp.cumsum(onehot, axis=0) - onehot) * onehot, axis=1)
    target = routed * capacity + position
    outgoing = jnp.zeros((experts * capacity, model_width), jnp.bfloat16).at[target].set(out_grad)
    arrived = lax.all_to_all(
        outgoing.reshape(experts, capacity, model_width),
        "expert",
        split_axis=0,
        concat_axis=0,
        tiled=True,
    )
    arrived = arrived.reshape(experts * capacity, model_width)
    weight = down_weight[0]
    own_rows = weight.shape[0]
    factor = 1.0 / math.sqrt(replicas * token_count)
    hidden_grad = lax.dot_general(
        arrived,
        lax.all_gather(weight, "dp", axis=0, tiled=True),
        (((1,), (1,)), ((), ())),
        preferred_element_type=jnp.float32,
    )
    pre_block = pre_act.astype(jnp.float32)
    pre_grad = (hidden_grad * derivative(pre_block)).astype(jnp.bfloat16)
    hidden = activate(pre_block).astype(jnp.bfloat16)
    summed = lax.psum_scatter(
        lax.dot_general(
            hidden, arrived, (((0,), (0,)), ((), ())), preferred_element_type=jnp.float32
        ),
        "dp",
        scatter_dimension=0,
        tiled=True,
    )
    return (pre_grad, (summed * factor).reshape(1, own_rows, model_width))


def solution(mesh):
    placed = (
        P(("dp", "expert"), None),
        P(("dp", "expert"), None),
        P(("dp", "expert"), None),
        P("expert", "dp", None),
    )
    return jax.shard_map(
        body,
        mesh=mesh,
        in_specs=placed,
        out_specs=(P(("dp", "expert"), None), P("expert", "dp", None)),
        check_vma=False,
    )
```
